512 devices in a mesh: seq: 128 (over z, y, core), head: 4 (over x).
Axes of the slice: x: 4, y: 4, z: 16, core: 2. Of those that a mesh axis runs over, the one named last changes fastest.
Arguments:
- queries: bfloat16 [65536, 2048], P('seq', 'head'), may hold values from -6 to 6
- key_vectors: bfloat16 [65536, 2048], P('seq', 'head'), may hold values from -6 to 6
- value_vectors: bfloat16 [65536, 2048], P('seq', 'head'), may hold values from -6 to 6
- gate_input: bfloat16 [65536, 2048], P('seq', 'head'), may hold values from -6 to 6
- out_weight: bfloat16 [2048, 4096], P('seq', 'head'), may hold values from -0.125 to 0.125
Outputs:
- layer_output: bfloat16 [65536, 4096], P('seq', 'head')
The draws below stay inside these ranges and needn't reach their ends.
All inputs are finite; a program needn't handle non-finite values.
Results may differ from the reference program's by a relative error of at most 0.0057.
Values may be sent and summed in bfloat16 or wider, within the bound.
No kernel may reach another device: no remote copies, remote signals or barrier semaphores. Data moves between devices by JAX's collectives and lax.ppermute only.
A program may use at most 64 MiB of HBM per device.

```python
import jax
import jax.numpy as jnp
from jax import lax

D = 4096
HD = 128
H = 16
TOK_DEV = 512
TOKENS = 65536


def block_levels(rng, shape, shards, smallest, largest):
    def one(position, blocks):
        draws = jax.random.uniform(jax.random.fold_in(jax.random.fold_in(rng, 6), position), (blocks,), jnp.float32, smallest / len(shards), largest / len(shards))
        return jnp.repeat(jnp.exp(draws), shape[position] // blocks).reshape((-1,) + (1,) * (len(shape) - position - 1))

    level = one(*shards[0])
    for cut in shards[1:]:
        level = level * one(*cut)
    return level


def normal_values(key, dims, scale, most, shards=(), kind=jnp.bfloat16):
    level = block_levels(key, dims, shards, -0.22, 0.18) if shards else 1.0
    values = jax.random.normal(key, dims, jnp.float32) * scale * level
    return jnp.minimum(jnp.maximum(values, -most), most).astype(kind)


def setup_inputs(seed: int = 0) -> dict:
    key_of = jax.random.split(jax.random.key(seed), 6)
    return {
        "queries": normal_values(key_of[0], (TOKENS, H * HD), 1.0, 6.0, ((0, 128), (1, 4))),
        "key_vectors": normal_values(key_of[1], (TOKENS, H * HD), 1.0, 6.0, ((0, 128), (1, 4))),
        "value_vectors": normal_values(key_of[2], (TOKENS, H * HD), 1.0, 6.0, ((0, 128), (1, 4))),
        "gate_input": normal_values(key_of[3], (TOKENS, H * HD), 1.0, 6.0, ((0, 128), (1, 4))),
        "out_weight": normal_values(key_of[4], (H * HD, D), (H * HD) ** -0.5, 0.125, ((0, 128), (1, 4))),
    }


def reference(queries, key_vectors, value_vectors, gate_input, out_weight):
    scale = HD ** (-0.5)
    blocks = TOKENS // TOK_DEV

    def shaped(array):
        return array.reshape(blocks, TOK_DEV, H * HD)
    rowpos = lax.broadcasted_iota(jnp.int32, (TOK_DEV, TOK_DEV), 0)
    colpos = lax.broadcasted_iota(jnp.int32, (TOK_DEV, TOK_DEV), 1)
    causal = colpos <= rowpos

    def block_step(carry, inputs):
        query_blk, key_blk, value_blk, gate_blk = inputs
        qhead = query_blk.reshape(TOK_DEV, H, HD).astype(jnp.float32)
        khead = key_blk.reshape(TOK_DEV, H, HD).astype(jnp.float32)
        vhead = value_blk.reshape(TOK_DEV, H, HD).astype(jnp.float32)
        scores = jnp.einsum('thd,shd->hts', qhead, khead) * scale
        scores = jnp.where(causal[None, :, :], scores, 0.0).astype(jnp.bfloat16)
        intra = jnp.einsum('hts,she->the', scores.astype(jnp.float32), vhead)
        rounded = carry.astype(jnp.bfloat16).astype(jnp.float32)
        inter = jnp.einsum('thd,hde->the', qhead, rounded) * scale
        attn = (intra + inter).reshape(TOK_DEV, H * HD)
        state = jnp.einsum('thd,the->hde', khead, vhead)
        mean_square = lax.optimization_barrier(jnp.mean(attn * attn, axis=1))
        hidden = (attn * jax.nn.silu(gate_blk.astype(jnp.float32))).astype(jnp.bfloat16)
        projected = jnp.dot(hidden, out_weight, preferred_element_type=jnp.float32)
        result = (projected * lax.rsqrt(mean_square + 1e-06)[:, None]).astype(jnp.bfloat16)
        return (carry + state, result)
    start = jnp.zeros((H, HD, HD), jnp.float32)
    final, outputs = lax.scan(block_step, start, (shaped(queries), shaped(key_vectors), shaped(value_vectors), shaped(gate_input)))
    return outputs.reshape(TOKENS, D)
```

```python
import functools

import jax
import jax.numpy as jnp
from jax import lax
from jax.experimental import pallas as pl
from jax.experimental.pallas import tpu as pltpu
from jax.sharding import Mesh
from jax.sharding import PartitionSpec as P

HD = 128
ZH, ZL, Y, C, X = "zh", "zl", "y", "c", "x"
SEQ = (ZH, ZL, Y, C)
NEAR = (ZL, Y, C)
F32 = jnp.float32
BF16 = jnp.bfloat16
VMEM = pl.BlockSpec(memory_space=pltpu.VMEM)
ANY = pl.BlockSpec(memory_space=pl.ANY)


def call(body, outs, n_in, flops, nbytes, in_specs=None, scratch=()):
    return pl.pallas_call(
        body,
        out_shape=outs,
        in_specs=in_specs or [VMEM] * n_in,
        out_specs=jax.tree.map(lambda _: VMEM, outs),
        scratch_shapes=list(scratch),
        cost_estimate=pl.CostEstimate(
            flops=flops, bytes_accessed=nbytes, transcendentals=0
        ),
        compiler_params=pltpu.CompilerParams(vmem_limit_bytes=40 * 2**20),
    )


def state_body(k_ref, v_ref, s_ref):
    for h in range(k_ref.shape[1] // HD):
        cols = slice(h * HD, (h + 1) * HD)
        s_ref[h] = lax.dot_general(
            k_ref[:, cols], v_ref[:, cols], (((0,), (0,)), ((), ())),
            preferred_element_type=F32,
        )


def local_body(q_ref, k_ref, v_ref, o_ref):
    rows = q_ref.shape[0]
    blk = 256
    scale = HD ** (-0.5)
    for h in range(q_ref.shape[1] // HD):
        cols = slice(h * HD, (h + 1) * HD)
        for i in range(rows // blk):
            r = slice(i * blk, (i + 1) * blk)
            seen = slice(0, (i + 1) * blk)
            s = lax.dot_general(
                q_ref[r, cols], k_ref[seen, cols], (((1,), (1,)), ((), ())),
                preferred_element_type=F32,
            ) * scale
            t_pos = i * blk + lax.broadcasted_iota(jnp.int32, s.shape, 0)
            s_pos = lax.broadcasted_iota(jnp.int32, s.shape, 1)
            s = jnp.where(s_pos <= t_pos, s, 0.0).astype(BF16)
            o_ref[r, cols] = jnp.dot(s, v_ref[seen, cols], preferred_element_type=F32)


def near_prefix_body(r_ref, e_ref, t_ref):
    acc = jnp.zeros(r_ref.shape[1:], F32)
    for j in range(r_ref.shape[0]):
        e_ref[j] = acc
        acc = acc + r_ref[j]
    for j in range(t_ref.shape[0]):
        t_ref[j] = acc


def far_prefix_body(e_ref, t_ref, p_ref):
    me = lax.axis_index(ZH)
    base = jnp.zeros(t_ref.shape[1:], F32)
    for j in range(t_ref.shape[0]):
        base = base + jnp.where(j < me, t_ref[j], 0.0)
    for j in range(e_ref.shape[0]):
        p_ref[j] = (e_ref[j] + base).astype(BF16)


def hidden_body(q_ref, p_ref, l_ref, g_ref, o_ref):
    rows, width = q_ref.shape
    scale = HD ** (-0.5)
    squares = jnp.zeros((rows, HD), F32)
    for h in range(width // HD):
        cols = slice(h * HD, (h + 1) * HD)
        inter = jnp.dot(q_ref[:, cols], p_ref[h], preferred_element_type=F32)
        attn = l_ref[:, cols] + inter * scale
        squares = squares + attn * attn
        gate = g_ref[:, cols].astype(F32)
        hid = (attn * (gate / (1.0 + jnp.exp(-gate)))).astype(BF16)
        for j in range(o_ref.shape[0]):
            o_ref[j, :rows, cols] = hid
    row = jnp.sum(squares.T, axis=0, keepdims=True)
    hi = row.astype(BF16).astype(F32)
    mid = (row - hi).astype(BF16).astype(F32)
    lo = row - hi - mid
    place = lax.broadcasted_iota(jnp.int32, (16, rows), 0)
    extra = jnp.where(place == 0, hi, jnp.where(place == 1, mid, jnp.where(place == 2, lo, 0.0)))
    for j in range(o_ref.shape[0]):
        o_ref[j, rows:, :] = extra.astype(BF16)


def project_body(h_ref, mine_ref, other_ref, o_ref, w_ref, sem):
    me = lax.axis_index(C)
    copies = []
    for y in range(mine_ref.shape[0]):
        for n, (src, core) in enumerate(((mine_ref, me), (other_ref, 1 - me))):
            copies.append(pltpu.make_async_copy(src.at[y], w_ref.at[:, y, core], sem.at[y, n]))
    for copy in copies:
        copy.start()
    rows, width = o_ref.shape
    parts = h_ref.shape[0]
    each = h_ref.shape[2]
    heads = each // HD
    row = jnp.zeros((1, rows), F32)
    for s in range(parts):
        for j in range(3):
            row = row + h_ref[s, rows + j : rows + j + 1, :].astype(F32)
    inv = lax.rsqrt(row / (parts * each) + 1e-06)
    inv = jnp.broadcast_to(inv, (HD, rows)).T
    for copy in copies:
        copy.wait()
    blk = 256
    for i in range(rows // blk):
        r = slice(i * blk, (i + 1) * blk)
        for n in range(width // 256):
            c = slice(n * 256, (n + 1) * 256)
            acc = jnp.zeros((blk, 256), F32)
            for s in range(parts):
                w = w_ref[s * heads : (s + 1) * heads, :, :, :, c].reshape(each, 256)
                acc = acc + jnp.dot(h_ref[s, r, :], w, preferred_element_type=F32)
            o_ref[r, c] = (acc * inv[r, :1]).astype(BF16)


def spread(block, axes):
    n = 1
    for a in axes:
        n *= lax.axis_size(a)
    return jnp.broadcast_to(block[None], (n, *block.shape))


def swap(array, axes):
    return lax.all_to_all(array, axes, 0, 0, tiled=True)


def per_device(queries, key_vectors, value_vectors, gate_input, out_weight):
    rows, width = queries.shape
    heads = width // HD
    near = lax.axis_size(ZL) * lax.axis_size(Y) * lax.axis_size(C)
    far = lax.axis_size(ZH)
    group = lax.axis_size(X)
    cols = out_weight.shape[1]
    piece = (heads * HD // near, HD)
    f32 = functools.partial(jax.ShapeDtypeStruct, dtype=F32)
    bf16 = functools.partial(jax.ShapeDtypeStruct, dtype=BF16)

    by_z = swap(spread(out_weight, (ZH, ZL)), (ZH, ZL))
    by_z = by_z.reshape(-1, *out_weight.shape)
    state = call(state_body, f32((heads, HD, HD)), 2, 10**8, 2**20)(key_vectors, value_vectors)
    local = call(local_body, f32((rows, width)), 3, 5 * 10**8, 2**21)(
        queries, key_vectors, value_vectors
    )
    pieces = swap(state.reshape(near, *piece), NEAR)
    earlier, total = call(
        near_prefix_body, (f32((near, *piece)), f32((far, *piece))), 1, 10**6, 2**19
    )(pieces)
    totals = swap(total, (ZH,))
    prefix = call(far_prefix_body, bf16((near, *piece)), 2, 10**6, 2**19)(earlier, totals)
    prefix = swap(prefix, NEAR).reshape(heads, HD, HD)
    hidden = call(
        hidden_body, bf16((group, rows + 16, width)), 4, 10**8, 2**22
    )(queries, prefix, local, gate_input)
    features = swap(hidden, (X,))
    by_y = swap(spread(by_z, (Y,)), (Y,)).reshape(-1, *by_z.shape)
    other = lax.ppermute(by_y, C, ((0, 1), (1, 0)))
    full = (by_z.shape[0], by_y.shape[0], 2, *out_weight.shape)
    return call(
        project_body, bf16((rows, cols)), 3, 2 * 10**9, 8 * 2**20,
        in_specs=[VMEM, ANY, ANY],
        scratch=[pltpu.VMEM(full, BF16), pltpu.SemaphoreType.DMA((by_y.shape[0], 2))],
    )(features, by_y, other)


def solution(mesh):
    torus = Mesh(
        mesh.devices.reshape(4, 4, 4, 2, mesh.shape["head"]), (ZH, ZL, Y, C, X)
    )
    return jax.shard_map(
        per_device,
        mesh=torus,
        in_specs=(P(SEQ, X),) * 5,
        out_specs=P(SEQ, X),
        check_vma=False,
    )
```

```python
import functools

import jax
import jax.numpy as jnp
from jax import lax
from jax.experimental import pallas as pl
from jax.experimental.pallas import tpu as pltpu
from jax.sharding import Mesh
from jax.sharding import PartitionSpec as P


HD = 128
ZH, ZL, Y, C, X = "zh", "zl", "y", "c", "x"
SEQ = (ZH, ZL, Y, C)
NEAR = (ZL, Y, C)
STEPS = (1, -1, 2)
NEXT = (0, 3, 1, 2)


F32 = jnp.float32
BF16 = jnp.bfloat16
VMEM = pl.BlockSpec(memory_space=pltpu.VMEM)
ANY = pl.BlockSpec(memory_space=pl.ANY)


def call(body, outs, n_in, flops, nbytes, in_specs=None, scratch=(), grant=16):
    return pl.pallas_call(
        body,
        out_shape=outs,
        in_specs=in_specs or [VMEM] * n_in,
        out_specs=jax.tree.map(lambda _: VMEM, outs),
        scratch_shapes=list(scratch),
        cost_estimate=pl.CostEstimate(
            flops=flops, bytes_accessed=nbytes, transcendentals=0
        ),
        compiler_params=pltpu.CompilerParams(vmem_limit_bytes=grant * 2**20),
    )


def state_body(k_ref, v_ref, s_ref):
    for h in range(k_ref.shape[1] // HD):
        cols = slice(h * HD, (h + 1) * HD)
        s_ref[h] = lax.dot_general(
            k_ref[:, cols], v_ref[:, cols], (((0,), (0,)), ((), ())),
            preferred_element_type=F32,
        )


def local_body(q_ref, k_ref, v_ref, o_ref):
    rows = q_ref.shape[0]
    blk = 256
    scale = HD ** (-0.5)
    for h in range(q_ref.shape[1] // HD):
        cols = slice(h * HD, (h + 1) * HD)
        for i in range(rows // blk):
            r = slice(i * blk, (i + 1) * blk)
            seen = slice(0, (i + 1) * blk)
            s = lax.dot_general(
                q_ref[r, cols], k_ref[seen, cols], (((1,), (1,)), ((), ())),
                preferred_element_type=F32,
            ) * scale
            t_pos = i * blk + lax.broadcasted_iota(jnp.int32, s.shape, 0)
            s_pos = lax.broadcasted_iota(jnp.int32, s.shape, 1)
            s = jnp.where(s_pos <= t_pos, s, 0.0).astype(BF16)
            o_ref[r, cols] = jnp.dot(s, v_ref[seen, cols], preferred_element_type=F32)


def near_prefix_body(r_ref, w_ref, e_ref, t_ref):
    acc = jnp.zeros(r_ref.shape[1:], F32)
    for j in range(r_ref.shape[0]):
        e_ref[j] = acc
        acc = acc + r_ref[j]
    hi = acc.astype(BF16)
    lo = (acc - hi.astype(F32)).astype(BF16)
    cols = w_ref.shape[1]
    for j in range(t_ref.shape[0]):
        t_ref[j, :, :cols] = w_ref[...]
        t_ref[j, :, cols : cols + HD] = hi
        t_ref[j, :, cols + HD :] = lo


def far_prefix_body(e_ref, t_ref, p_ref, w_ref):
    me = lax.axis_index(ZH)
    cols = w_ref.shape[2]
    base = jnp.zeros(e_ref.shape[1:], F32)
    for j in range(t_ref.shape[0]):
        hi = t_ref[j, :, cols : cols + HD].astype(F32)
        lo = t_ref[j, :, cols + HD :].astype(F32)
        base = base + jnp.where(j < me, hi + lo, 0.0)
        w_ref[j] = t_ref[j, :, :cols]
    for j in range(e_ref.shape[0]):
        p_ref[j] = (e_ref[j] + base).astype(BF16)


def hidden_body(q_ref, p_ref, l_ref, g_ref, o_ref):
    rows, width = q_ref.shape
    scale = HD ** (-0.5)
    squares = jnp.zeros((rows, HD), F32)
    for h in range(width // HD):
        cols = slice(h * HD, (h + 1) * HD)
        inter = jnp.dot(q_ref[:, cols], p_ref[h], preferred_element_type=F32)
        attn = l_ref[:, cols] + inter * scale
        squares = squares + attn * attn
        gate = g_ref[:, cols].astype(F32)
        hid = (attn * (gate / (1.0 + jnp.exp(-gate)))).astype(BF16)
        for j in range(o_ref.shape[0]):
            o_ref[j, :rows, cols] = hid
    row = jnp.sum(squares.T, axis=0, keepdims=True)
    hi = row.astype(BF16).astype(F32)
    mid = (row - hi).astype(BF16).astype(F32)
    lo = row - hi - mid
    place = lax.broadcasted_iota(jnp.int32, (16, rows), 0)
    extra = jnp.where(place == 0, hi, jnp.where(place == 1, mid, jnp.where(place == 2, lo, 0.0)))
    for j in range(o_ref.shape[0]):
        o_ref[j, rows:, :] = extra.astype(BF16)


def project_body(h_ref, *refs):
    blocks = refs[:8]
    o_ref, w_ref, sem = refs[8:]
    core = lax.axis_index(C)
    zl = lax.axis_index(ZL)
    y = lax.axis_index(Y)
    copies = []
    for n, block in enumerate(blocks):
        owner = core if n < 4 else 1 - core
        for k in range(4):
            outer, inner = NEXT[n % 4], NEXT[k]
            by_z = jnp.where(owner == 0, inner, outer)
            by_y = jnp.where(owner == 0, outer, inner)
            to = w_ref.at[:, lax.rem(zl + by_z, 4), lax.rem(y + by_y, 4), owner]
            copies.append(pltpu.make_async_copy(block.at[k], to, sem.at[n, k]))
    for copy in copies:
        copy.start()
    rows, width = o_ref.shape
    parts = h_ref.shape[0]
    each = h_ref.shape[2]
    row = jnp.zeros((1, rows), F32)
    for s in range(parts):
        for j in range(3):
            row = row + h_ref[s, rows + j : rows + j + 1, :].astype(F32)
    inv = lax.rsqrt(row / (parts * each) + 1e-06)
    inv = jnp.broadcast_to(inv, (HD, rows)).T
    for copy in copies:
        copy.wait()
    blk = 256
    for i in range(rows // blk):
        r = slice(i * blk, (i + 1) * blk)
        for n in range(width // 256):
            c = slice(n * 256, (n + 1) * 256)
            acc = jnp.zeros((blk, 256), F32)
            for s in range(parts):
                w = w_ref[s, :, :, :, :, c].reshape(each, 256)
                acc = acc + jnp.dot(h_ref[s, r, :], w, preferred_element_type=F32)
            o_ref[r, c] = (acc * inv[r, :1]).astype(BF16)


def swap(array, axes):
    return lax.all_to_all(array, axes, 0, 0, tiled=True)


def moved(array, first, second, step):
    pairs = []
    n = {a: lax.axis_size(a) for a in SEQ}
    ring = n[ZH] * n[ZL]
    for z in range(ring):
        for y in range(n[Y]):
            for c in range(n[C]):
                to_z, to_y = z, y
                if (first, second)[c] == "z":
                    hop = step if step != 2 or z % 2 == 0 else -2
                    to_z = (z + hop) % ring
                else:
                    to_y = (y + step) % n[Y]
                pairs.append(((z * n[Y] + y) * n[C] + c, (to_z * n[Y] + to_y) * n[C] + c))
    return lax.ppermute(array, SEQ, pairs)


def per_device(queries, key_vectors, value_vectors, gate_input, out_weight):
    rows, width = queries.shape
    heads = width // HD
    near = lax.axis_size(ZL) * lax.axis_size(Y) * lax.axis_size(C)
    far = lax.axis_size(ZH)
    group = lax.axis_size(X)
    cols = out_weight.shape[1]
    piece = (heads * HD // near, HD)
    f32 = functools.partial(jax.ShapeDtypeStruct, dtype=F32)
    bf16 = functools.partial(jax.ShapeDtypeStruct, dtype=BF16)

    state = call(state_body, f32((heads, HD, HD)), 2, 10**8, 2**20)(
        key_vectors, value_vectors
    )
    local = call(local_body, f32((rows, width)), 3, 5 * 10**8, 2**21)(
        queries, key_vectors, value_vectors
    )
    pieces = swap(state.reshape(near, *piece), NEAR)
    earlier, total = call(
        near_prefix_body,
        (f32((near, *piece)), bf16((far, piece[0], cols + 2 * HD))),
        2, 10**6, 2**19,
    )(pieces, out_weight)
    totals = swap(total, (ZH,))
    prefix, w_far = call(
        far_prefix_body,
        (bf16((near, *piece)), bf16((far, *out_weight.shape))),
        2, 10**6, 2**19,
    )(earlier, totals)
    prefix = swap(prefix, NEAR).reshape(heads, HD, HD)
    hidden = call(
        hidden_body, bf16((group, rows + 16, width)), 4, 10**8, 2**22
    )(queries, prefix, local, gate_input)
    features = swap(hidden, (X,))
    first = [w_far]
    for step in STEPS:
        first.append(moved(w_far, "z", "y", step))
    first = jnp.stack(first)
    mine = [first]
    for step in STEPS:
        mine.append(moved(first, "y", "z", step))
    other = []
    for block in mine:
        other.append(lax.ppermute(block, C, ((0, 1), (1, 0))))
    full = (far, lax.axis_size(ZL), lax.axis_size(Y), 2, *out_weight.shape)
    return call(
        project_body, bf16((rows, cols)), 3, 2 * 10**9, 8 * 2**20,
        in_specs=[VMEM] + [ANY] * 8,
        grant=60,
        scratch=[pltpu.VMEM(full, BF16), pltpu.SemaphoreType.DMA((8, 4))],
    )(features, *mine, *other)


def solution(mesh):
    torus = Mesh(
        mesh.devices.reshape(4, 4, 4, 2, mesh.shape["head"]), (ZH, ZL, Y, C, X)
    )
    return jax.shard_map(
        per_device,
        mesh=torus,
        in_specs=(P(SEQ, X),) * 5,
        out_specs=P(SEQ, X),
        check_vma=False,
    )
```

```python
import functools

import jax
import jax.numpy as jnp
from jax import lax
from jax.experimental import pallas as pl
from jax.experimental.pallas import tpu as pltpu
from jax.sharding import Mesh
from jax.sharding import PartitionSpec as P


HD = 128
ZH, ZL, Y, C, X = "zh", "zl", "y", "c", "x"
SEQ = (ZH, ZL, Y, C)
NEAR = (ZL, Y, C)
STEPS = (1, -1, 2)
NEXT = (0, 3, 1, 2)


F32 = jnp.float32
BF16 = jnp.bfloat16
VMEM = pl.BlockSpec(memory_space=pltpu.VMEM)
ANY = pl.BlockSpec(memory_space=pl.ANY)


def call(body, outs, n_in, flops, nbytes, in_specs=None, scratch=(), grant=16):
    return pl.pallas_call(
        body,
        out_shape=outs,
        in_specs=in_specs or [VMEM] * n_in,
        out_specs=jax.tree.map(lambda _: VMEM, outs),
        scratch_shapes=list(scratch),
        cost_estimate=pl.CostEstimate(
            flops=flops, bytes_accessed=nbytes, transcendentals=0
        ),
        compiler_params=pltpu.CompilerParams(vmem_limit_bytes=grant * 2**20),
    )


def state_body(k_ref, v_ref, s_ref):
    for h in range(k_ref.shape[1] // HD):
        cols = slice(h * HD, (h + 1) * HD)
        s_ref[h] = lax.dot_general(
            k_ref[:, cols], v_ref[:, cols], (((0,), (0,)), ((), ())),
            preferred_element_type=F32,
        )


def local_body(q_ref, k_ref, v_ref, o_ref):
    rows = q_ref.shape[0]
    blk = 256
    scale = HD ** (-0.5)
    for h in range(q_ref.shape[1] // HD):
        cols = slice(h * HD, (h + 1) * HD)
        for i in range(rows // blk):
            r = slice(i * blk, (i + 1) * blk)
            seen = slice(0, (i + 1) * blk)
            s = lax.dot_general(
                q_ref[r, cols], k_ref[seen, cols], (((1,), (1,)), ((), ())),
                preferred_element_type=F32,
            ) * scale
            t_pos = i * blk + lax.broadcasted_iota(jnp.int32, s.shape, 0)
            s_pos = lax.broadcasted_iota(jnp.int32, s.shape, 1)
            s = jnp.where(s_pos <= t_pos, s, 0.0).astype(BF16)
            o_ref[r, cols] = jnp.dot(s, v_ref[seen, cols], preferred_element_type=F32)


def near_prefix_body(r_ref, w_ref, e_ref, t_ref):
    acc = jnp.zeros(r_ref.shape[1:], F32)
    for j in range(r_ref.shape[0]):
        e_ref[j] = acc
        acc = acc + r_ref[j]
    hi = acc.astype(BF16)
    lo = (acc - hi.astype(F32)).astype(BF16)
    cols = w_ref.shape[1]
    for j in range(t_ref.shape[0]):
        t_ref[j, :, :cols] = w_ref[...]
        t_ref[j, :, cols : cols + HD] = hi
        t_ref[j, :, cols + HD :] = lo


def far_prefix_body(e_ref, t_ref, p_ref, w_ref):
    me = lax.axis_index(ZH)
    cols = w_ref.shape[2]
    base = jnp.zeros(e_ref.shape[1:], F32)
    for j in range(t_ref.shape[0]):
        hi = t_ref[j, :, cols : cols + HD].astype(F32)
        lo = t_ref[j, :, cols + HD :].astype(F32)
        base = base + jnp.where(j < me, hi + lo, 0.0)
        w_ref[j] = t_ref[j, :, :cols]
    for j in range(e_ref.shape[0]):
        p_ref[j] = (e_ref[j] + base).astype(BF16)


def hidden_body(q_ref, p_ref, l_ref, g_ref, o_ref):
    rows, width = q_ref.shape
    scale = HD ** (-0.5)
    squares = jnp.zeros((rows, HD), F32)
    for h in range(width // HD):
        cols = slice(h * HD, (h + 1) * HD)
        inter = jnp.dot(q_ref[:, cols], p_ref[h], preferred_element_type=F32)
        attn = l_ref[:, cols] + inter * scale
        squares = squares + attn * attn
        gate = g_ref[:, cols].astype(F32)
        hid = (attn * (gate / (1.0 + jnp.exp(-gate)))).astype(BF16)
        for j in range(o_ref.shape[0]):
            o_ref[j, :rows, cols] = hid
    row = jnp.sum(squares.T, axis=0, keepdims=True)
    hi = row.astype(BF16).astype(F32)
    mid = (row - hi).astype(BF16).astype(F32)
    lo = row - hi - mid
    place = lax.broadcasted_iota(jnp.int32, (16, rows), 0)
    extra = jnp.where(place == 0, hi, jnp.where(place == 1, mid, jnp.where(place == 2, lo, 0.0)))
    for j in range(o_ref.shape[0]):
        o_ref[j, rows:, :] = extra.astype(BF16)


def assemble_body(*refs):
    blocks = refs[:8]
    w_ref, sem = refs[8:]
    core = lax.axis_index(C)
    zl = lax.axis_index(ZL)
    y = lax.axis_index(Y)
    copies = []
    for n, block in enumerate(blocks):
        owner = core if n < 4 else 1 - core
        for k in range(4):
            outer, inner = NEXT[n % 4], NEXT[k]
            by_z = jnp.where(owner == 0, inner, outer)
            by_y = jnp.where(owner == 0, outer, inner)
            to = w_ref.at[:, lax.rem(zl + by_z, 4), lax.rem(y + by_y, 4), owner]
            copies.append(pltpu.make_async_copy(block.at[k], to, sem.at[n, k]))
    for copy in copies:
        copy.start()
    for copy in copies:
        copy.wait()


def project_body(h_ref, w_ref, o_ref):
    rows, width = o_ref.shape
    parts = h_ref.shape[0]
    each = h_ref.shape[2]
    row = jnp.zeros((1, rows), F32)
    for s in range(parts):
        for j in range(3):
            row = row + h_ref[s, rows + j : rows + j + 1, :].astype(F32)
    inv = lax.rsqrt(row / (parts * each) + 1e-06)
    inv = jnp.broadcast_to(inv, (HD, rows)).T
    blk = 256
    for i in range(rows // blk):
        r = slice(i * blk, (i + 1) * blk)
        for n in range(width // 256):
            c = slice(n * 256, (n + 1) * 256)
            acc = jnp.zeros((blk, 256), F32)
            for s in range(parts):
                w = w_ref[s, :, :, :, :, c].reshape(each, 256)
                acc = acc + jnp.dot(h_ref[s, r, :], w, preferred_element_type=F32)
            o_ref[r, c] = (acc * inv[r, :1]).astype(BF16)


def swap(array, axes):
    return lax.all_to_all(array, axes, 0, 0, tiled=True)


def moved(array, first, second, step):
    pairs = []
    n = {a: lax.axis_size(a) for a in SEQ}
    ring = n[ZH] * n[ZL]
    for z in range(ring):
        for y in range(n[Y]):
            for c in range(n[C]):
                to_z, to_y = z, y
                if (first, second)[c] == "z":
                    hop = step if step != 2 or z % 2 == 0 else -2
                    to_z = (z + hop) % ring
                else:
                    to_y = (y + step) % n[Y]
                pairs.append(((z * n[Y] + y) * n[C] + c, (to_z * n[Y] + to_y) * n[C] + c))
    return lax.ppermute(array, SEQ, pairs)


def per_device(queries, key_vectors, value_vectors, gate_input, out_weight):
    rows, width = queries.shape
    heads = width // HD
    near = lax.axis_size(ZL) * lax.axis_size(Y) * lax.axis_size(C)
    far = lax.axis_size(ZH)
    group = lax.axis_size(X)
    cols = out_weight.shape[1]
    piece = (heads * HD // near, HD)
    f32 = functools.partial(jax.ShapeDtypeStruct, dtype=F32)
    bf16 = functools.partial(jax.ShapeDtypeStruct, dtype=BF16)

    state = call(state_body, f32((heads, HD, HD)), 2, 10**8, 2**20)(
        key_vectors, value_vectors
    )
    local = call(local_body, f32((rows, width)), 3, 5 * 10**8, 2**21)(
        queries, key_vectors, value_vectors
    )
    pieces = swap(state.reshape(near, *piece), NEAR)
    earlier, total = call(
        near_prefix_body,
        (f32((near, *piece)), bf16((far, piece[0], cols + 2 * HD))),
        2, 10**6, 2**19,
    )(pieces, out_weight)
    totals = swap(total, (ZH,))
    prefix, w_far = call(
        far_prefix_body,
        (bf16((near, *piece)), bf16((far, *out_weight.shape))),
        2, 10**6, 2**19,
    )(earlier, totals)
    prefix = swap(prefix, NEAR).reshape(heads, HD, HD)
    hidden = call(
        hidden_body, bf16((group, rows + 16, width)), 4, 10**8, 2**22
    )(queries, prefix, local, gate_input)
    features = swap(hidden, (X,))
    first = [w_far]
    for step in STEPS:
        first.append(moved(w_far, "z", "y", step))
    first = jnp.stack(first)
    mine = [first]
    for step in STEPS:
        mine.append(moved(first, "y", "z", step))
    other = []
    for block in mine:
        other.append(lax.ppermute(block, C, ((0, 1), (1, 0))))
    full = (far, lax.axis_size(ZL), lax.axis_size(Y), 2, *out_weight.shape)
    weight = call(
        assemble_body, bf16(full), 8, 10**6, 8 * 2**20,
        in_specs=[ANY] * 8,
        scratch=[pltpu.SemaphoreType.DMA((8, 4))],
    )(*mine, *other)
    return call(
        project_body, bf16((rows, cols)), 2, 2 * 10**9, 8 * 2**20
    )(features, weight)


def solution(mesh):
    torus = Mesh(
        mesh.devices.reshape(4, 4, 4, 2, mesh.shape["head"]), (ZH, ZL, Y, C, X)
    )
    return jax.shard_map(
        per_device,
        mesh=torus,
        in_specs=(P(SEQ, X),) * 5,
        out_specs=P(SEQ, X),
        check_vma=False,
    )
```

```python
import functools

import jax
import jax.numpy as jnp
from jax import lax
from jax.experimental import pallas as pl
from jax.experimental.pallas import tpu as pltpu
from jax.sharding import Mesh
from jax.sharding import PartitionSpec as P


HD = 128
ZH, ZL, Y, C, X = "zh", "zl", "y", "c", "x"
SEQ = (ZH, ZL, Y, C)
NEAR = (ZL, Y, C)
STEPS = (1, -1, 2)
NEXT = (0, 3, 1, 2)


F32 = jnp.float32
BF16 = jnp.bfloat16
VMEM = pl.BlockSpec(memory_space=pltpu.VMEM)
ANY = pl.BlockSpec(memory_space=pl.ANY)


def call(body, outs, n_in, flops, nbytes, in_specs=None, out_spec=VMEM, scratch=(), grant=16):
    return pl.pallas_call(
        body,
        out_shape=outs,
        in_specs=in_specs or [VMEM] * n_in,
        out_specs=jax.tree.map(lambda _: out_spec, outs),
        scratch_shapes=list(scratch),
        cost_estimate=pl.CostEstimate(
            flops=flops, bytes_accessed=nbytes, transcendentals=0
        ),
        compiler_params=pltpu.CompilerParams(vmem_limit_bytes=grant * 2**20),
    )


def state_body(k_hbm, v_hbm, w_hbm, s_ref, w_ref, k_ref, v_ref, sem):
    copies = [
        pltpu.make_async_copy(k_hbm, k_ref, sem.at[0]),
        pltpu.make_async_copy(v_hbm, v_ref, sem.at[1]),
        pltpu.make_async_copy(w_hbm, w_ref, sem.at[2]),
    ]
    for copy in copies:
        copy.start()
    copies[0].wait()
    copies[1].wait()
    for h in range(k_ref.shape[1] // HD):
        cols = slice(h * HD, (h + 1) * HD)
        s_ref[h] = lax.dot_general(
            k_ref[:, cols], v_ref[:, cols], (((0,), (0,)), ((), ())),
            preferred_element_type=F32,
        )
    copies[2].wait()


def local_body(q_ref, k_ref, v_ref, o_ref):
    rows = q_ref.shape[0]
    blk = 256
    scale = HD ** (-0.5)
    for h in range(q_ref.shape[1] // HD):
        cols = slice(h * HD, (h + 1) * HD)
        for i in range(rows // blk):
            r = slice(i * blk, (i + 1) * blk)
            seen = slice(0, (i + 1) * blk)
            s = lax.dot_general(
                q_ref[r, cols], k_ref[seen, cols], (((1,), (1,)), ((), ())),
                preferred_element_type=F32,
            ) * scale
            t_pos = i * blk + lax.broadcasted_iota(jnp.int32, s.shape, 0)
            s_pos = lax.broadcasted_iota(jnp.int32, s.shape, 1)
            s = jnp.where(s_pos <= t_pos, s, 0.0).astype(BF16)
            o_ref[r, cols] = jnp.dot(s, v_ref[seen, cols], preferred_element_type=F32)


def near_prefix_body(r_ref, w_ref, e_ref, t_ref):
    acc = jnp.zeros(r_ref.shape[1:], F32)
    for j in range(r_ref.shape[0]):
        e_ref[j] = acc
        acc = acc + r_ref[j]
    hi = acc.astype(BF16)
    lo = (acc - hi.astype(F32)).astype(BF16)
    cols = w_ref.shape[1]
    for j in range(t_ref.shape[0]):
        t_ref[j, :, :cols] = w_ref[...]
        t_ref[j, :, cols : cols + HD] = hi
        t_ref[j, :, cols + HD :] = lo


def far_prefix_body(e_ref, t_ref, p_ref, w_ref):
    me = lax.axis_index(ZH)
    cols = w_ref.shape[2]
    base = jnp.zeros(e_ref.shape[1:], F32)
    for j in range(t_ref.shape[0]):
        hi = t_ref[j, :, cols : cols + HD].astype(F32)
        lo = t_ref[j, :, cols + HD :].astype(F32)
        base = base + jnp.where(j < me, hi + lo, 0.0)
        w_ref[j] = t_ref[j, :, :cols]
    for j in range(e_ref.shape[0]):
        p_ref[j] = (e_ref[j] + base).astype(BF16)


def hidden_body(q_ref, p_ref, l_ref, g_ref, o_ref):
    rows, width = q_ref.shape
    scale = HD ** (-0.5)
    squares = jnp.zeros((rows, HD), F32)
    for h in range(width // HD):
        cols = slice(h * HD, (h + 1) * HD)
        inter = jnp.dot(q_ref[:, cols], p_ref[h], preferred_element_type=F32)
        attn = l_ref[:, cols] + inter * scale
        squares = squares + attn * attn
        hid = (attn * g_ref[:, cols]).astype(BF16)
        for j in range(o_ref.shape[0]):
            o_ref[j, :rows, cols] = hid
    row = jnp.sum(squares.T, axis=0, keepdims=True)
    hi = row.astype(BF16).astype(F32)
    mid = (row - hi).astype(BF16).astype(F32)
    lo = row - hi - mid
    place = lax.broadcasted_iota(jnp.int32, (16, rows), 0)
    extra = jnp.where(place == 0, hi, jnp.where(place == 1, mid, jnp.where(place == 2, lo, 0.0)))
    for j in range(o_ref.shape[0]):
        o_ref[j, rows:, :] = extra.astype(BF16)


def assemble_body(*refs):
    blocks = refs[:4]
    w_ref, sem = refs[4:]
    core = lax.axis_index(C)
    zl = lax.axis_index(ZL)
    y = lax.axis_index(Y)
    copies = []
    for n, block in enumerate(blocks):
        for k in range(4):
            outer, inner = NEXT[n], NEXT[k]
            by_z = jnp.where(core == 0, inner, outer)
            by_y = jnp.where(core == 0, outer, inner)
            to = w_ref.at[:, lax.rem(zl + by_z, 4), lax.rem(y + by_y, 4)]
            copies.append(pltpu.make_async_copy(block.at[k], to, sem.at[n, k]))
    for copy in copies:
        copy.start()
    for copy in copies:
        copy.wait()


def project_body(h_hbm, mine_ref, other_ref, out_ref, h_ref, w_ref, acc_ref, o_ref, sem, out_sem):
    rows, width = o_ref.shape
    parts = h_ref.shape[0]
    each = h_ref.shape[2]
    core = lax.axis_index(C)
    span = w_ref.shape[0] // parts
    tile = 256
    copies = []
    for s in range(parts):
        part = slice(s * span, (s + 1) * span)
        copies.append(
            [
                pltpu.make_async_copy(h_hbm.at[s], h_ref.at[s], sem.at[s, 0]),
                pltpu.make_async_copy(mine_ref.at[part], w_ref.at[part, core], sem.at[s, 1]),
                pltpu.make_async_copy(other_ref.at[part], w_ref.at[part, 1 - core], sem.at[s, 2]),
            ]
        )
        for copy in copies[s]:
            copy.start()
    for s in range(parts):
        for copy in copies[s]:
            copy.wait()
        last = s == parts - 1
        if last:
            row = jnp.zeros((1, rows), F32)
            for p in range(parts):
                for j in range(3):
                    row = row + h_ref[p, rows + j : rows + j + 1, :].astype(F32)
            inv = lax.rsqrt(row / (parts * each) + 1e-06)
            inv = jnp.broadcast_to(inv, (HD, rows)).T
        block = rows // 2 if last else rows
        for i in range(rows // block):
            r = slice(i * block, (i + 1) * block)
            for n in range(width // tile):
                c = slice(n * tile, (n + 1) * tile)
                w = w_ref[s * span : (s + 1) * span, :, :, c].reshape(each, tile)
                acc = jnp.dot(h_ref[s, r, :], w, preferred_element_type=F32)
                if s > 0:
                    acc = acc + acc_ref[r, c]
                if last:
                    o_ref[r, c] = (acc * inv[r, :1]).astype(BF16)
                else:
                    acc_ref[r, c] = acc
            if last:
                pltpu.make_async_copy(o_ref.at[r], out_ref.at[r], out_sem.at[i]).start()
    for i in range(2):
        r = slice(i * (rows // 2), (i + 1) * (rows // 2))
        pltpu.make_async_copy(o_ref.at[r], out_ref.at[r], out_sem.at[i]).wait()


def gate_body(g_ref, o_ref):
    gate = g_ref[...].astype(F32)
    o_ref[...] = gate / (1.0 + jnp.exp(-gate))


def swap(array, axes):
    return lax.all_to_all(array, axes, 0, 0, tiled=True)


def moved(array, first, second, step):
    pairs = []
    n = {a: lax.axis_size(a) for a in SEQ}
    ring = n[ZH] * n[ZL]
    for z in range(ring):
        for y in range(n[Y]):
            for c in range(n[C]):
                to_z, to_y = z, y
                if (first, second)[c] == "z":
                    hop = step if step != 2 or z % 2 == 0 else -2
                    to_z = (z + hop) % ring
                else:
                    to_y = (y + step) % n[Y]
                pairs.append(((z * n[Y] + y) * n[C] + c, (to_z * n[Y] + to_y) * n[C] + c))
    return lax.ppermute(array, SEQ, pairs)


def per_device(queries, key_vectors, value_vectors, gate_input, out_weight):
    rows, width = queries.shape
    heads = width // HD
    near = lax.axis_size(ZL) * lax.axis_size(Y) * lax.axis_size(C)
    far = lax.axis_size(ZH)
    group = lax.axis_size(X)
    cols = out_weight.shape[1]
    piece = (heads * HD // near, HD)
    f32 = functools.partial(jax.ShapeDtypeStruct, dtype=F32)
    bf16 = functools.partial(jax.ShapeDtypeStruct, dtype=BF16)

    state, w_own = call(
        state_body, (f32((heads, HD, HD)), bf16(out_weight.shape)), 3, 10**8, 2**20,
        in_specs=[ANY] * 3,
        scratch=[pltpu.VMEM((rows, width), BF16)] * 2 + [pltpu.SemaphoreType.DMA((3,))],
        grant=58,
    )(key_vectors, value_vectors, out_weight)
    local = call(local_body, f32((rows, width)), 3, 5 * 10**8, 2**21)(
        queries, key_vectors, value_vectors
    )
    gate = call(gate_body, f32((rows, width)), 1, 10**6, 2**20)(gate_input)
    pieces = swap(state.reshape(near, *piece), NEAR)
    earlier, total = call(
        near_prefix_body,
        (f32((near, *piece)), bf16((far, piece[0], cols + 2 * HD))),
        2, 10**6, 2**19,
    )(pieces, w_own)
    totals = swap(total, (ZH,))
    prefix, w_far = call(
        far_prefix_body,
        (bf16((near, *piece)), bf16((far, *out_weight.shape))),
        2, 10**6, 2**19,
    )(earlier, totals)
    prefix = swap(prefix, NEAR).reshape(heads, HD, HD)
    hidden = call(
        hidden_body, bf16((group, rows + 16, width)), 4, 10**8, 2**22
    )(queries, prefix, local, gate)
    features = swap(hidden, (X,))
    first = [w_far]
    for step in STEPS:
        first.append(moved(w_far, "z", "y", step))
    *first, _ = lax.optimization_barrier((*first, hidden))
    first = jnp.stack(first)
    mine = [first]
    for step in STEPS:
        mine.append(moved(first, "y", "z", step))
    half = (far, lax.axis_size(ZL), lax.axis_size(Y), *out_weight.shape)
    weight = call(
        assemble_body, bf16(half), 4, 10**6, 4 * 2**20,
        in_specs=[ANY] * 4,
        out_spec=ANY,
        scratch=[pltpu.SemaphoreType.DMA((4, 4))],
    )(*mine)
    other = lax.ppermute(weight, C, ((0, 1), (1, 0)))
    flat = (-1, *out_weight.shape)
    count = half[0] * half[1] * half[2]
    return call(
        project_body, bf16((rows, cols)), 3, 2 * 10**9, 8 * 2**20,
        in_specs=[ANY] * 3,
        out_spec=ANY,
        scratch=[
            pltpu.VMEM((group, rows + 16, width), BF16),
            pltpu.VMEM((count, 2, *out_weight.shape), BF16),
            pltpu.VMEM((rows, cols), F32),
            pltpu.VMEM((rows, cols), BF16),
            pltpu.SemaphoreType.DMA((group, 3)),
            pltpu.SemaphoreType.DMA((2,)),
        ],
        grant=60,
    )(features, weight.reshape(flat), other.reshape(flat))


def solution(mesh):
    torus = Mesh(
        mesh.devices.reshape(4, 4, 4, 2, mesh.shape["head"]), (ZH, ZL, Y, C, X)
    )
    return jax.shard_map(
        per_device,
        mesh=torus,
        in_specs=(P(SEQ, X),) * 5,
        out_specs=P(SEQ, X),
        check_vma=False,
    )
```

```python
import functools

import jax
import jax.numpy as jnp
from jax import lax
from jax.experimental import pallas as pl
from jax.experimental.pallas import tpu as pltpu
from jax.sharding import Mesh
from jax.sharding import PartitionSpec as P


HD = 128
ZH, ZL, Y, C, X = "zh", "zl", "y", "c", "x"
SEQ = (ZH, ZL, Y, C)
NEAR = (ZL, Y, C)
STEPS = (1, -1, 2)
NEXT = (0, 3, 1, 2)


F32 = jnp.float32
BF16 = jnp.bfloat16
VMEM = pl.BlockSpec(memory_space=pltpu.VMEM)
ANY = pl.BlockSpec(memory_space=pl.ANY)


def call(body, outs, n_in, flops, nbytes, in_specs=None, out_spec=VMEM, scratch=(), grant=16):
    return pl.pallas_call(
        body,
        out_shape=outs,
        in_specs=in_specs or [VMEM] * n_in,
        out_specs=jax.tree.map(lambda _: out_spec, outs),
        scratch_shapes=list(scratch),
        cost_estimate=pl.CostEstimate(
            flops=flops, bytes_accessed=nbytes, transcendentals=0
        ),
        compiler_params=pltpu.CompilerParams(vmem_limit_bytes=grant * 2**20),
    )


def state_body(k_hbm, v_hbm, w_hbm, s_ref, w_ref, k_ref, v_ref, sem):
    copies = [
        pltpu.make_async_copy(k_hbm, k_ref, sem.at[0]),
        pltpu.make_async_copy(v_hbm, v_ref, sem.at[1]),
        pltpu.make_async_copy(w_hbm, w_ref, sem.at[2]),
    ]
    for copy in copies:
        copy.start()
    copies[0].wait()
    copies[1].wait()
    for h in range(k_ref.shape[1] // HD):
        cols = slice(h * HD, (h + 1) * HD)
        s_ref[h] = lax.dot_general(
            k_ref[:, cols], v_ref[:, cols], (((0,), (0,)), ((), ())),
            preferred_element_type=F32,
        )
    copies[2].wait()


def local_body(q_ref, k_ref, v_ref, o_ref):
    rows = q_ref.shape[0]
    blk = 256
    scale = HD ** (-0.5)
    for h in range(q_ref.shape[1] // HD):
        cols = slice(h * HD, (h + 1) * HD)
        for i in range(rows // blk):
            r = slice(i * blk, (i + 1) * blk)
            seen = slice(0, (i + 1) * blk)
            s = lax.dot_general(
                q_ref[r, cols], k_ref[seen, cols], (((1,), (1,)), ((), ())),
                preferred_element_type=F32,
            ) * scale
            t_pos = i * blk + lax.broadcasted_iota(jnp.int32, s.shape, 0)
            s_pos = lax.broadcasted_iota(jnp.int32, s.shape, 1)
            s = jnp.where(s_pos <= t_pos, s, 0.0).astype(BF16)
            o_ref[r, cols] = jnp.dot(s, v_ref[seen, cols], preferred_element_type=F32)


def near_prefix_body(r_ref, w_ref, e_ref, t_ref):
    acc = jnp.zeros(r_ref.shape[1:], F32)
    for j in range(r_ref.shape[0]):
        e_ref[j] = acc
        acc = acc + r_ref[j]
    hi = acc.astype(BF16)
    lo = (acc - hi.astype(F32)).astype(BF16)
    cols = w_ref.shape[1]
    for j in range(t_ref.shape[0]):
        t_ref[j, :, :cols] = w_ref[...]
        t_ref[j, :, cols : cols + HD] = hi
        t_ref[j, :, cols + HD :] = lo


def far_prefix_body(e_ref, t_ref, p_ref, w_ref):
    me = lax.axis_index(ZH)
    cols = w_ref.shape[2]
    base = jnp.zeros(e_ref.shape[1:], F32)
    for j in range(t_ref.shape[0]):
        hi = t_ref[j, :, cols : cols + HD].astype(F32)
        lo = t_ref[j, :, cols + HD :].astype(F32)
        base = base + jnp.where(j < me, hi + lo, 0.0)
        w_ref[j] = t_ref[j, :, :cols]
    for j in range(e_ref.shape[0]):
        p_ref[j] = (e_ref[j] + base).astype(BF16)


def hidden_body(q_ref, p_ref, l_ref, g_ref, o_ref):
    rows, width = q_ref.shape
    scale = HD ** (-0.5)
    squares = jnp.zeros((rows, HD), F32)
    for h in range(width // HD):
        cols = slice(h * HD, (h + 1) * HD)
        inter = jnp.dot(q_ref[:, cols], p_ref[h], preferred_element_type=F32)
        attn = l_ref[:, cols] + inter * scale
        squares = squares + attn * attn
        hid = (attn * g_ref[:, cols]).astype(BF16)
        for j in range(o_ref.shape[0]):
            o_ref[j, :rows, cols] = hid
    row = jnp.sum(squares.T, axis=0, keepdims=True)
    hi = row.astype(BF16).astype(F32)
    mid = (row - hi).astype(BF16).astype(F32)
    lo = row - hi - mid
    place = lax.broadcasted_iota(jnp.int32, (16, rows), 0)
    extra = jnp.where(place == 0, hi, jnp.where(place == 1, mid, jnp.where(place == 2, lo, 0.0)))
    for j in range(o_ref.shape[0]):
        o_ref[j, rows:, :] = extra.astype(BF16)


def assemble_body(*refs):
    blocks = refs[:4]
    w_ref, sem = refs[4:]
    core = lax.axis_index(C)
    zl = lax.axis_index(ZL)
    y = lax.axis_index(Y)
    copies = []
    for n, block in enumerate(blocks):
        for k in range(4):
            outer, inner = NEXT[n], NEXT[k]
            by_z = jnp.where(core == 1, inner, outer)
            by_y = jnp.where(core == 1, outer, inner)
            to = w_ref.at[:, lax.rem(zl + by_z, 4), lax.rem(y + by_y, 4)]
            copies.append(pltpu.make_async_copy(block.at[k], to, sem.at[n, k]))
    for copy in copies:
        copy.start()
    for copy in copies:
        copy.wait()


def project_body(h_hbm, mine_ref, other_ref, out_ref, h_ref, w_ref, acc_ref, o_ref, sem, out_sem):
    rows, width = o_ref.shape
    parts = h_ref.shape[0]
    each = h_ref.shape[2]
    core = lax.axis_index(C)
    span = w_ref.shape[0] // parts
    tile = 256
    copies = []
    for s in range(parts):
        part = slice(s * span, (s + 1) * span)
        copies.append(
            [
                pltpu.make_async_copy(h_hbm.at[s], h_ref.at[s], sem.at[s, 0]),
                pltpu.make_async_copy(mine_ref.at[part], w_ref.at[part, core], sem.at[s, 1]),
                pltpu.make_async_copy(other_ref.at[part], w_ref.at[part, 1 - core], sem.at[s, 2]),
            ]
        )
        for copy in copies[s]:
            copy.start()
    for s in range(parts):
        for copy in copies[s]:
            copy.wait()
        last = s == parts - 1
        if last:
            row = jnp.zeros((1, rows), F32)
            for p in range(parts):
                for j in range(3):
                    row = row + h_ref[p, rows + j : rows + j + 1, :].astype(F32)
            inv = lax.rsqrt(row / (parts * each) + 1e-06)
            inv = jnp.broadcast_to(inv, (HD, rows)).T
        block = rows // 2 if last else rows
        for i in range(rows // block):
            r = slice(i * block, (i + 1) * block)
            for n in range(width // tile):
                c = slice(n * tile, (n + 1) * tile)
                w = w_ref[s * span : (s + 1) * span, :, :, c].reshape(each, tile)
                acc = jnp.dot(h_ref[s, r, :], w, preferred_element_type=F32)
                if s > 0:
                    acc = acc + acc_ref[r, c]
                if last:
                    o_ref[r, c] = (acc * inv[r, :1]).astype(BF16)
                else:
                    acc_ref[r, c] = acc
            if last:
                pltpu.make_async_copy(o_ref.at[r], out_ref.at[r], out_sem.at[i]).start()
    for i in range(2):
        r = slice(i * (rows // 2), (i + 1) * (rows // 2))
        pltpu.make_async_copy(o_ref.at[r], out_ref.at[r], out_sem.at[i]).wait()


def gate_body(g_ref, o_ref):
    gate = g_ref[...].astype(F32)
    o_ref[...] = gate / (1.0 + jnp.exp(-gate))


def swap(array, axes):
    return lax.all_to_all(array, axes, 0, 0, tiled=True)


def moved(array, first, second, step):
    pairs = []
    n = {a: lax.axis_size(a) for a in SEQ}
    ring = n[ZH] * n[ZL]
    for z in range(ring):
        for y in range(n[Y]):
            for c in range(n[C]):
                to_z, to_y = z, y
                if (first, second)[c] == "z":
                    hop = step if step != 2 or z % 2 == 0 else -2
                    to_z = (z + hop) % ring
                else:
                    to_y = (y + step) % n[Y]
                pairs.append(((z * n[Y] + y) * n[C] + c, (to_z * n[Y] + to_y) * n[C] + c))
    return lax.ppermute(array, SEQ, pairs)


def per_device(queries, key_vectors, value_vectors, gate_input, out_weight):
    rows, width = queries.shape
    heads = width // HD
    near = lax.axis_size(ZL) * lax.axis_size(Y) * lax.axis_size(C)
    far = lax.axis_size(ZH)
    group = lax.axis_size(X)
    cols = out_weight.shape[1]
    piece = (heads * HD // near, HD)
    f32 = functools.partial(jax.ShapeDtypeStruct, dtype=F32)
    bf16 = functools.partial(jax.ShapeDtypeStruct, dtype=BF16)

    state, w_own = call(
        state_body, (f32((heads, HD, HD)), bf16(out_weight.shape)), 3, 10**8, 2**20,
        in_specs=[ANY] * 3,
        scratch=[pltpu.VMEM((rows, width), BF16)] * 2 + [pltpu.SemaphoreType.DMA((3,))],
        grant=58,
    )(key_vectors, value_vectors, out_weight)
    local = call(local_body, f32((rows, width)), 3, 5 * 10**8, 2**21)(
        queries, key_vectors, value_vectors
    )
    gate = call(gate_body, f32((rows, width)), 1, 10**6, 2**20)(gate_input)
    pieces = swap(state.reshape(near, *piece), NEAR)
    earlier, total = call(
        near_prefix_body,
        (f32((near, *piece)), bf16((far, piece[0], cols + 2 * HD))),
        2, 10**6, 2**19,
    )(pieces, w_own)
    totals = swap(total, (ZH,))
    prefix, w_far = call(
        far_prefix_body,
        (bf16((near, *piece)), bf16((far, *out_weight.shape))),
        2, 10**6, 2**19,
    )(earlier, totals)
    prefix = swap(prefix, NEAR).reshape(heads, HD, HD)
    hidden = call(
        hidden_body, bf16((group, rows + 16, width)), 4, 10**8, 2**22
    )(queries, prefix, local, gate)
    features = swap(hidden, (X,))
    first = [w_far]
    for step in STEPS:
        first.append(moved(w_far, "y", "z", step))
    *first, _ = lax.optimization_barrier((*first, hidden))
    first = jnp.stack(first)
    mine = [first]
    for step in STEPS:
        mine.append(moved(first, "z", "y", step))
    half = (far, lax.axis_size(ZL), lax.axis_size(Y), *out_weight.shape)
    weight = call(
        assemble_body, bf16(half), 4, 10**6, 4 * 2**20,
        in_specs=[ANY] * 4,
        out_spec=ANY,
        scratch=[pltpu.SemaphoreType.DMA((4, 4))],
    )(*mine)
    other = lax.ppermute(weight, C, ((0, 1), (1, 0)))
    flat = (-1, *out_weight.shape)
    count = half[0] * half[1] * half[2]
    return call(
        project_body, bf16((rows, cols)), 3, 2 * 10**9, 8 * 2**20,
        in_specs=[ANY] * 3,
        out_spec=ANY,
        scratch=[
            pltpu.VMEM((group, rows + 16, width), BF16),
            pltpu.VMEM((count, 2, *out_weight.shape), BF16),
            pltpu.VMEM((rows, cols), F32),
            pltpu.VMEM((rows, cols), BF16),
            pltpu.SemaphoreType.DMA((group, 3)),
            pltpu.SemaphoreType.DMA((2,)),
        ],
        grant=60,
    )(features, weight.reshape(flat), other.reshape(flat))


def solution(mesh):
    torus = Mesh(
        mesh.devices.reshape(4, 4, 4, 2, mesh.shape["head"]), (ZH, ZL, Y, C, X)
    )
    return jax.shard_map(
        per_device,
        mesh=torus,
        in_specs=(P(SEQ, X),) * 5,
        out_specs=P(SEQ, X),
        check_vma=False,
    )
```

```python
import functools

import jax
import jax.numpy as jnp
from jax import lax
from jax.experimental import pallas as pl
from jax.experimental.pallas import tpu as pltpu
from jax.sharding import Mesh
from jax.sharding import PartitionSpec as P


HD = 128
ZH, ZL, Y, C, X = "zh", "zl", "y", "c", "x"
SEQ = (ZH, ZL, Y, C)
NEAR = (ZL, Y, C)
STEPS = (1, -1, 2)
PLACES = ((0, 3), (1, 2))
NEXT = (0, 3, 1, 2)


F32 = jnp.float32
BF16 = jnp.bfloat16
VMEM = pl.BlockSpec(memory_space=pltpu.VMEM)
ANY = pl.BlockSpec(memory_space=pl.ANY)


def call(body, outs, n_in, flops, nbytes, in_specs=None, out_spec=VMEM, scratch=(), grant=16):
    return pl.pallas_call(
        body,
        out_shape=outs,
        in_specs=in_specs or [VMEM] * n_in,
        out_specs=jax.tree.map(lambda _: out_spec, outs),
        scratch_shapes=list(scratch),
        cost_estimate=pl.CostEstimate(
            flops=flops, bytes_accessed=nbytes, transcendentals=0
        ),
        compiler_params=pltpu.CompilerParams(vmem_limit_bytes=grant * 2**20),
    )


def state_body(k_hbm, v_hbm, w_hbm, s_ref, w_ref, k_ref, v_ref, sem):
    copies = [
        pltpu.make_async_copy(k_hbm, k_ref, sem.at[0]),
        pltpu.make_async_copy(v_hbm, v_ref, sem.at[1]),
        pltpu.make_async_copy(w_hbm, w_ref, sem.at[2]),
    ]
    for copy in copies:
        copy.start()
    copies[0].wait()
    copies[1].wait()
    for h in range(k_ref.shape[1] // HD):
        cols = slice(h * HD, (h + 1) * HD)
        s_ref[h] = lax.dot_general(
            k_ref[:, cols], v_ref[:, cols], (((0,), (0,)), ((), ())),
            preferred_element_type=F32,
        )
    copies[2].wait()


def local_body(q_ref, k_ref, v_ref, o_ref):
    rows = q_ref.shape[0]
    blk = 256
    scale = HD ** (-0.5)
    for h in range(q_ref.shape[1] // HD):
        cols = slice(h * HD, (h + 1) * HD)
        for i in range(rows // blk):
            r = slice(i * blk, (i + 1) * blk)
            seen = slice(0, (i + 1) * blk)
            s = lax.dot_general(
                q_ref[r, cols], k_ref[seen, cols], (((1,), (1,)), ((), ())),
                preferred_element_type=F32,
            ) * scale
            t_pos = i * blk + lax.broadcasted_iota(jnp.int32, s.shape, 0)
            s_pos = lax.broadcasted_iota(jnp.int32, s.shape, 1)
            s = jnp.where(s_pos <= t_pos, s, 0.0).astype(BF16)
            o_ref[r, cols] = jnp.dot(s, v_ref[seen, cols], preferred_element_type=F32)


def near_prefix_body(r_ref, w_ref, e_ref, t_ref):
    acc = jnp.zeros(r_ref.shape[1:], F32)
    for j in range(r_ref.shape[0]):
        e_ref[j] = acc
        acc = acc + r_ref[j]
    hi = acc.astype(BF16)
    lo = (acc - hi.astype(F32)).astype(BF16)
    cols = w_ref.shape[1]
    for j in range(t_ref.shape[0]):
        t_ref[j, :, :cols] = w_ref[...]
        t_ref[j, :, cols : cols + HD] = hi
        t_ref[j, :, cols + HD :] = lo


def far_prefix_body(e_ref, t_ref, p_ref, w_ref):
    me = lax.axis_index(ZH)
    cols = w_ref.shape[2]
    base = jnp.zeros(e_ref.shape[1:], F32)
    for j in range(t_ref.shape[0]):
        hi = t_ref[j, :, cols : cols + HD].astype(F32)
        lo = t_ref[j, :, cols + HD :].astype(F32)
        base = base + jnp.where(j < me, hi + lo, 0.0)
        w_ref[j] = t_ref[j, :, :cols]
    for j in range(e_ref.shape[0]):
        p_ref[j] = (e_ref[j] + base).astype(BF16)


def hidden_body(q_ref, p_ref, l_ref, g_ref, out_ref, o_ref, sem):
    rows, width = q_ref.shape
    scale = HD ** (-0.5)
    half = rows // 2
    sums = []
    copies = []
    for i in range(2):
        r = slice(i * half, (i + 1) * half)
        squares = jnp.zeros((half, HD), F32)
        for h in range(width // HD):
            cols = slice(h * HD, (h + 1) * HD)
            inter = jnp.dot(q_ref[r, cols], p_ref[h], preferred_element_type=F32)
            attn = l_ref[r, cols] + inter * scale
            squares = squares + attn * attn
            o_ref[r, cols] = (attn * g_ref[r, cols]).astype(BF16)
        sums.append(jnp.sum(squares.T, axis=0, keepdims=True))
        if i == 1:
            row = jnp.concatenate(sums, axis=1)
            hi = row.astype(BF16).astype(F32)
            mid = (row - hi).astype(BF16).astype(F32)
            lo = row - hi - mid
            place = lax.broadcasted_iota(jnp.int32, (16, rows), 0)
            extra = jnp.where(
                place == 0, hi, jnp.where(place == 1, mid, jnp.where(place == 2, lo, 0.0))
            )
            o_ref[rows:, :] = extra.astype(BF16)
            r = slice(half, rows + 16)
        for j in range(out_ref.shape[0]):
            copies.append(pltpu.make_async_copy(o_ref.at[r], out_ref.at[j, r], sem.at[i, j]))
            copies[-1].start()
    for copy in copies:
        copy.wait()


def assemble_body(*refs):
    blocks = refs[:2]
    w_ref, sem = refs[2:]
    mine = jnp.where(lax.axis_index(C) == 1, lax.axis_index(ZL), lax.axis_index(Y))
    copies = []
    for n, block in enumerate(blocks):
        for k in range(4):
            to = w_ref.at[n, :, lax.rem(mine + NEXT[k], 4)]
            copies.append(pltpu.make_async_copy(block.at[k], to, sem.at[n, k]))
    for copy in copies:
        copy.start()
    for copy in copies:
        copy.wait()


def project_body(h_hbm, *refs):
    pieces = refs[:4]
    out_ref, h_ref, w_ref, acc_ref, o_ref, sem, out_sem = refs[4:]
    rows, width = o_ref.shape
    parts = h_ref.shape[0]
    each = h_ref.shape[2]
    core = lax.axis_index(C)
    zl = lax.axis_index(ZL)
    y = lax.axis_index(Y)
    tile = 256
    copies = []
    for s in range(parts):
        copies.append([pltpu.make_async_copy(h_hbm.at[s], h_ref.at[s], sem.at[s, 16])])
        copies[s][0].start()
        for p, piece in enumerate(pieces):
            owner = core if p < 2 else 1 - core
            for n in range(2):
                step = NEXT[PLACES[p % 2][n]]
                down = w_ref.at[s, :, lax.rem(y + step, 4), owner]
                along = w_ref.at[s, lax.rem(zl + step, 4), :, owner]
                by_y = pltpu.make_async_copy(piece.at[n, s], down, sem.at[s, 2 * p + n])
                by_z = pltpu.make_async_copy(piece.at[n, s], along, sem.at[s, 8 + 2 * p + n])
                copies[s].append((owner, by_y, by_z))

                @pl.when(owner == 1)
                def _():
                    by_y.start()

                @pl.when(owner == 0)
                def _():
                    by_z.start()

    for s in range(parts):
        copies[s][0].wait()
        for owner, by_y, by_z in copies[s][1:]:
            @pl.when(owner == 1)
            def _():
                by_y.wait()

            @pl.when(owner == 0)
            def _():
                by_z.wait()

        last = s == parts - 1
        if last:
            row = jnp.zeros((1, rows), F32)
            for p in range(parts):
                for j in range(3):
                    row = row + h_ref[p, rows + j : rows + j + 1, :].astype(F32)
            inv = lax.rsqrt(row / (parts * each) + 1e-06)
            inv = jnp.broadcast_to(inv, (HD, rows)).T
        block = rows // 2 if last else rows
        for i in range(rows // block):
            r = slice(i * block, (i + 1) * block)
            for n in range(width // tile):
                c = slice(n * tile, (n + 1) * tile)
                w = w_ref[s, :, :, :, :, c].reshape(each, tile)
                acc = jnp.dot(h_ref[s, r, :], w, preferred_element_type=F32)
                if s > 0:
                    acc = acc + acc_ref[r, c]
                if last:
                    o_ref[r, c] = (acc * inv[r, :1]).astype(BF16)
                else:
                    acc_ref[r, c] = acc
            if last:
                pltpu.make_async_copy(o_ref.at[r], out_ref.at[r], out_sem.at[i]).start()
    for i in range(2):
        r = slice(i * (rows // 2), (i + 1) * (rows // 2))
        pltpu.make_async_copy(o_ref.at[r], out_ref.at[r], out_sem.at[i]).wait()


def gate_body(g_ref, o_ref):
    gate = g_ref[...].astype(F32)
    o_ref[...] = gate / (1.0 + jnp.exp(-gate))


def swap(array, axes):
    return lax.all_to_all(array, axes, 0, 0, tiled=True)


def moved(array, first, second, step):
    pairs = []
    n = {a: lax.axis_size(a) for a in SEQ}
    ring = n[ZH] * n[ZL]
    for z in range(ring):
        for y in range(n[Y]):
            for c in range(n[C]):
                to_z, to_y = z, y
                if (first, second)[c] == "z":
                    hop = step if step != 2 or z % 2 == 0 else -2
                    to_z = (z + hop) % ring
                else:
                    to_y = (y + step) % n[Y]
                pairs.append(((z * n[Y] + y) * n[C] + c, (to_z * n[Y] + to_y) * n[C] + c))
    return lax.ppermute(array, SEQ, pairs)


def per_device(queries, key_vectors, value_vectors, gate_input, out_weight):
    rows, width = queries.shape
    heads = width // HD
    near = lax.axis_size(ZL) * lax.axis_size(Y) * lax.axis_size(C)
    far = lax.axis_size(ZH)
    group = lax.axis_size(X)
    cols = out_weight.shape[1]
    piece = (heads * HD // near, HD)
    f32 = functools.partial(jax.ShapeDtypeStruct, dtype=F32)
    bf16 = functools.partial(jax.ShapeDtypeStruct, dtype=BF16)

    state, w_own = call(
        state_body, (f32((heads, HD, HD)), bf16(out_weight.shape)), 3, 10**8, 2**20,
        in_specs=[ANY] * 3,
        scratch=[pltpu.VMEM((rows, width), BF16)] * 2 + [pltpu.SemaphoreType.DMA((3,))],
        grant=58,
    )(key_vectors, value_vectors, out_weight)
    local = call(local_body, f32((rows, width)), 3, 5 * 10**8, 2**21)(
        queries, key_vectors, value_vectors
    )
    gate = call(gate_body, f32((rows, width)), 1, 10**6, 2**20)(gate_input)
    pieces = swap(state.reshape(near, *piece), NEAR)
    earlier, total = call(
        near_prefix_body,
        (f32((near, *piece)), bf16((far, piece[0], cols + 2 * HD))),
        2, 10**6, 2**19,
    )(pieces, w_own)
    totals = swap(total, (ZH,))
    prefix, w_far = call(
        far_prefix_body,
        (bf16((near, *piece)), bf16((far, *out_weight.shape))),
        2, 10**6, 2**19,
    )(earlier, totals)
    prefix = swap(prefix, NEAR).reshape(heads, HD, HD)
    hidden = call(
        hidden_body, bf16((group, rows + 16, width)), 4, 10**8, 2**22,
        out_spec=ANY,
        scratch=[
            pltpu.VMEM((rows + 16, width), BF16),
            pltpu.SemaphoreType.DMA((2, group)),
        ],
    )(queries, prefix, local, gate)
    features = swap(hidden, (X,))
    first = [w_far]
    for step in STEPS:
        first.append(moved(w_far, "y", "z", step))
    *first, _ = lax.optimization_barrier((*first, hidden))
    first = jnp.stack(first)
    mine = [first]
    for step in STEPS:
        mine.append(moved(first, "z", "y", step))
    halves = []
    for places in PLACES:
        halves.append(
            call(
                assemble_body, bf16((2, far, 4, *out_weight.shape)),
                2, 10**6, 2 * 2**20,
                in_specs=[ANY] * 2,
                out_spec=ANY,
                scratch=[pltpu.SemaphoreType.DMA((2, 4))],
            )(*[mine[k] for k in places])
        )
    for n in range(2):
        halves.append(lax.ppermute(halves[n], C, ((0, 1), (1, 0))))
    return call(
        project_body, bf16((rows, cols)), 5, 2 * 10**9, 8 * 2**20,
        in_specs=[ANY] * 5,
        out_spec=ANY,
        scratch=[
            pltpu.VMEM((group, rows + 16, width), BF16),
            pltpu.VMEM((far, 4, 4, 2, *out_weight.shape), BF16),
            pltpu.VMEM((rows, cols), F32),
            pltpu.VMEM((rows, cols), BF16),
            pltpu.SemaphoreType.DMA((group, 17)),
            pltpu.SemaphoreType.DMA((2,)),
        ],
        grant=60,
    )(features, *halves)


def solution(mesh):
    torus = Mesh(
        mesh.devices.reshape(4, 4, 4, 2, mesh.shape["head"]), (ZH, ZL, Y, C, X)
    )
    return jax.shard_map(
        per_device,
        mesh=torus,
        in_specs=(P(SEQ, X),) * 5,
        out_specs=P(SEQ, X),
        check_vma=False,
    )
```

```python
import functools

import jax
import jax.numpy as jnp
from jax import lax
from jax.experimental import pallas as pl
from jax.experimental.pallas import tpu as pltpu
from jax.sharding import Mesh
from jax.sharding import PartitionSpec as P


HD = 128
ZH, ZL, Y, C, X = "zh", "zl", "y", "c", "x"
SEQ = (ZH, ZL, Y, C)
NEAR = (ZL, Y, C)
STEPS = (1, -1, 2)
PLACES = ((0, 3), (1, 2))
NEXT = (0, 3, 1, 2)


F32 = jnp.float32
BF16 = jnp.bfloat16
VMEM = pl.BlockSpec(memory_space=pltpu.VMEM)
ANY = pl.BlockSpec(memory_space=pl.ANY)


def call(body, outs, n_in, flops, nbytes, in_specs=None, out_spec=VMEM, scratch=(), grant=16):
    return pl.pallas_call(
        body,
        out_shape=outs,
        in_specs=in_specs or [VMEM] * n_in,
        out_specs=jax.tree.map(lambda _: out_spec, outs),
        scratch_shapes=list(scratch),
        cost_estimate=pl.CostEstimate(
            flops=flops, bytes_accessed=nbytes, transcendentals=0
        ),
        compiler_params=pltpu.CompilerParams(vmem_limit_bytes=grant * 2**20),
    )


def state_body(k_hbm, v_hbm, w_hbm, s_ref, w_ref, k_ref, v_ref, sem):
    copies = [
        pltpu.make_async_copy(k_hbm, k_ref, sem.at[0]),
        pltpu.make_async_copy(v_hbm, v_ref, sem.at[1]),
        pltpu.make_async_copy(w_hbm, w_ref, sem.at[2]),
    ]
    for copy in copies:
        copy.start()
    copies[0].wait()
    copies[1].wait()
    for h in range(k_ref.shape[1] // HD):
        cols = slice(h * HD, (h + 1) * HD)
        s_ref[h] = lax.dot_general(
            k_ref[:, cols], v_ref[:, cols], (((0,), (0,)), ((), ())),
            preferred_element_type=F32,
        )
    copies[2].wait()


def local_body(q_ref, k_ref, v_ref, o_ref):
    rows = q_ref.shape[0]
    blk = 256
    scale = HD ** (-0.5)
    for h in range(q_ref.shape[1] // HD):
        cols = slice(h * HD, (h + 1) * HD)
        for i in range(rows // blk):
            r = slice(i * blk, (i + 1) * blk)
            seen = slice(0, (i + 1) * blk)
            s = lax.dot_general(
                q_ref[r, cols], k_ref[seen, cols], (((1,), (1,)), ((), ())),
                preferred_element_type=F32,
            ) * scale
            t_pos = i * blk + lax.broadcasted_iota(jnp.int32, s.shape, 0)
            s_pos = lax.broadcasted_iota(jnp.int32, s.shape, 1)
            s = jnp.where(s_pos <= t_pos, s, 0.0).astype(BF16)
            o_ref[r, cols] = jnp.dot(s, v_ref[seen, cols], preferred_element_type=F32)


def near_prefix_body(r_ref, w_ref, e_ref, t_ref):
    acc = jnp.zeros(r_ref.shape[1:], F32)
    for j in range(r_ref.shape[0]):
        e_ref[j] = acc
        acc = acc + r_ref[j]
    hi = acc.astype(BF16)
    lo = (acc - hi.astype(F32)).astype(BF16)
    cols = w_ref.shape[1]
    for j in range(t_ref.shape[0]):
        t_ref[j, :, :cols] = w_ref[...]
        t_ref[j, :, cols : cols + HD] = hi
        t_ref[j, :, cols + HD :] = lo


def far_prefix_body(e_ref, t_ref, p_ref, w_ref):
    me = lax.axis_index(ZH)
    cols = w_ref.shape[2]
    base = jnp.zeros(e_ref.shape[1:], F32)
    for j in range(t_ref.shape[0]):
        hi = t_ref[j, :, cols : cols + HD].astype(F32)
        lo = t_ref[j, :, cols + HD :].astype(F32)
        base = base + jnp.where(j < me, hi + lo, 0.0)
        w_ref[j] = t_ref[j, :, :cols]
    for j in range(e_ref.shape[0]):
        p_ref[j] = (e_ref[j] + base).astype(BF16)


def hidden_body(q_ref, p_ref, l_ref, g_ref, out_ref, o_ref, sem):
    rows, width = q_ref.shape
    scale = HD ** (-0.5)
    half = rows // 2
    sums = []
    copies = []
    for i in range(2):
        r = slice(i * half, (i + 1) * half)
        squares = jnp.zeros((half, HD), F32)
        for h in range(width // HD):
            cols = slice(h * HD, (h + 1) * HD)
            inter = jnp.dot(q_ref[r, cols], p_ref[h], preferred_element_type=F32)
            attn = l_ref[r, cols] + inter * scale
            squares = squares + attn * attn
            o_ref[r, cols] = (attn * g_ref[r, cols]).astype(BF16)
        sums.append(jnp.sum(squares.T, axis=0, keepdims=True))
        if i == 1:
            row = jnp.concatenate(sums, axis=1)
            hi = row.astype(BF16).astype(F32)
            mid = (row - hi).astype(BF16).astype(F32)
            lo = row - hi - mid
            place = lax.broadcasted_iota(jnp.int32, (16, rows), 0)
            extra = jnp.where(
                place == 0, hi, jnp.where(place == 1, mid, jnp.where(place == 2, lo, 0.0))
            )
            o_ref[rows:, :] = extra.astype(BF16)
            r = slice(half, rows + 16)
        for j in range(out_ref.shape[0]):
            copies.append(pltpu.make_async_copy(o_ref.at[r], out_ref.at[j, r], sem.at[i, j]))
            copies[-1].start()
    for copy in copies:
        copy.wait()


def assemble_body(*refs):
    blocks = refs[:2]
    w_ref, sem = refs[2:]
    mine = jnp.where(lax.axis_index(C) == 1, lax.axis_index(ZL), lax.axis_index(Y))
    copies = []
    for n, block in enumerate(blocks):
        for k in range(4):
            to = w_ref.at[n, :, lax.rem(mine + NEXT[k], 4)]
            copies.append(pltpu.make_async_copy(block.at[k], to, sem.at[n, k]))
    for copy in copies:
        copy.start()
    for copy in copies:
        copy.wait()


def project_body(h_hbm, *refs):
    pieces = refs[:4]
    out_ref, h_ref, w_ref, acc_ref, o_ref, sem, out_sem = refs[4:]
    rows, width = o_ref.shape
    parts = h_ref.shape[0]
    each = h_ref.shape[2]
    core = lax.axis_index(C)
    zl = lax.axis_index(ZL)
    y = lax.axis_index(Y)
    tile = 256

    def fetch(s, p, n, owner, along):
        step = NEXT[PLACES[p % 2][n]]
        if along:
            to = w_ref.at[s, lax.rem(zl + step, 4), :, owner]
        else:
            to = w_ref.at[s, :, lax.rem(y + step, 4), owner]
        return pltpu.make_async_copy(pieces[p].at[n, s], to, sem.at[s, 2 * p + n])

    def part(s):
        return pltpu.make_async_copy(h_hbm.at[s], h_ref.at[s], sem.at[s, 8])

    def start(me):
        for s in range(parts):
            part(s).start()
            for p in range(4):
                owner = me if p < 2 else 1 - me
                for n in range(2):
                    fetch(s, p, n, owner, owner == 0).start()

    @pl.when(core == 0)
    def _():
        start(0)

    @pl.when(core == 1)
    def _():
        start(1)

    for s in range(parts):
        part(s).wait()
        for p in range(4):
            for n in range(2):
                fetch(s, p, n, 0, True).wait()
        last = s == parts - 1
        if last:
            row = jnp.zeros((1, rows), F32)
            for p in range(parts):
                for j in range(3):
                    row = row + h_ref[p, rows + j : rows + j + 1, :].astype(F32)
            inv = lax.rsqrt(row / (parts * each) + 1e-06)
            inv = jnp.broadcast_to(inv, (HD, rows)).T
        block = rows // 2 if last else rows
        for i in range(rows // block):
            r = slice(i * block, (i + 1) * block)
            for n in range(width // tile):
                c = slice(n * tile, (n + 1) * tile)
                w = w_ref[s, :, :, :, :, c].reshape(each, tile)
                acc = jnp.dot(h_ref[s, r, :], w, preferred_element_type=F32)
                if s > 0:
                    acc = acc + acc_ref[r, c]
                if last:
                    o_ref[r, c] = (acc * inv[r, :1]).astype(BF16)
                else:
                    acc_ref[r, c] = acc
            if last:
                pltpu.make_async_copy(o_ref.at[r], out_ref.at[r], out_sem.at[i]).start()
    for i in range(2):
        r = slice(i * (rows // 2), (i + 1) * (rows // 2))
        pltpu.make_async_copy(o_ref.at[r], out_ref.at[r], out_sem.at[i]).wait()


def gate_body(g_ref, o_ref):
    gate = g_ref[...].astype(F32)
    o_ref[...] = gate / (1.0 + jnp.exp(-gate))


def swap(array, axes):
    return lax.all_to_all(array, axes, 0, 0, tiled=True)


def moved(array, first, second, step):
    pairs = []
    n = {a: lax.axis_size(a) for a in SEQ}
    ring = n[ZH] * n[ZL]
    for z in range(ring):
        for y in range(n[Y]):
            for c in range(n[C]):
                to_z, to_y = z, y
                if (first, second)[c] == "z":
                    hop = step if step != 2 or z % 2 == 0 else -2
                    to_z = (z + hop) % ring
                else:
                    to_y = (y + step) % n[Y]
                pairs.append(((z * n[Y] + y) * n[C] + c, (to_z * n[Y] + to_y) * n[C] + c))
    return lax.ppermute(array, SEQ, pairs)


def per_device(queries, key_vectors, value_vectors, gate_input, out_weight):
    rows, width = queries.shape
    heads = width // HD
    near = lax.axis_size(ZL) * lax.axis_size(Y) * lax.axis_size(C)
    far = lax.axis_size(ZH)
    group = lax.axis_size(X)
    cols = out_weight.shape[1]
    piece = (heads * HD // near, HD)
    f32 = functools.partial(jax.ShapeDtypeStruct, dtype=F32)
    bf16 = functools.partial(jax.ShapeDtypeStruct, dtype=BF16)

    state, w_own = call(
        state_body, (f32((heads, HD, HD)), bf16(out_weight.shape)), 3, 10**8, 2**20,
        in_specs=[ANY] * 3,
        scratch=[pltpu.VMEM((rows, width), BF16)] * 2 + [pltpu.SemaphoreType.DMA((3,))],
        grant=58,
    )(key_vectors, value_vectors, out_weight)
    local = call(local_body, f32((rows, width)), 3, 5 * 10**8, 2**21)(
        queries, key_vectors, value_vectors
    )
    gate = call(gate_body, f32((rows, width)), 1, 10**6, 2**20)(gate_input)
    pieces = swap(state.reshape(near, *piece), NEAR)
    earlier, total = call(
        near_prefix_body,
        (f32((near, *piece)), bf16((far, piece[0], cols + 2 * HD))),
        2, 10**6, 2**19,
    )(pieces, w_own)
    totals = swap(total, (ZH,))
    prefix, w_far = call(
        far_prefix_body,
        (bf16((near, *piece)), bf16((far, *out_weight.shape))),
        2, 10**6, 2**19,
    )(earlier, totals)
    prefix = swap(prefix, NEAR).reshape(heads, HD, HD)
    hidden = call(
        hidden_body, bf16((group, rows + 16, width)), 4, 10**8, 2**22,
        out_spec=ANY,
        scratch=[
            pltpu.VMEM((rows + 16, width), BF16),
            pltpu.SemaphoreType.DMA((2, group)),
        ],
    )(queries, prefix, local, gate)
    features = swap(hidden, (X,))
    first = [w_far]
    for step in STEPS:
        first.append(moved(w_far, "y", "z", step))
    *first, _ = lax.optimization_barrier((*first, hidden))
    first = jnp.stack(first)
    mine = [first]
    for step in STEPS:
        mine.append(moved(first, "z", "y", step))
    halves = []
    for places in PLACES:
        halves.append(
            call(
                assemble_body, bf16((2, far, 4, *out_weight.shape)),
                2, 10**6, 2 * 2**20,
                in_specs=[ANY] * 2,
                out_spec=ANY,
                scratch=[pltpu.SemaphoreType.DMA((2, 4))],
            )(*[mine[k] for k in places])
        )
    for n in range(2):
        halves.append(lax.ppermute(halves[n], C, ((0, 1), (1, 0))))
    return call(
        project_body, bf16((rows, cols)), 5, 2 * 10**9, 8 * 2**20,
        in_specs=[ANY] * 5,
        out_spec=ANY,
        scratch=[
            pltpu.VMEM((group, rows + 16, width), BF16),
            pltpu.VMEM((far, 4, 4, 2, *out_weight.shape), BF16),
            pltpu.VMEM((rows, cols), F32),
            pltpu.VMEM((rows, cols), BF16),
            pltpu.SemaphoreType.DMA((group, 9)),
            pltpu.SemaphoreType.DMA((2,)),
        ],
        grant=60,
    )(features, *halves)


def solution(mesh):
    torus = Mesh(
        mesh.devices.reshape(4, 4, 4, 2, mesh.shape["head"]), (ZH, ZL, Y, C, X)
    )
    return jax.shard_map(
        per_device,
        mesh=torus,
        in_specs=(P(SEQ, X),) * 5,
        out_specs=P(SEQ, X),
        check_vma=False,
    )
```
